32 devices in a mesh: expert: 4 (over z), shard: 8 (over y, x, core).
Axes of the slice: x: 2, y: 2, z: 4, core: 2. Of those that a mesh axis runs over, the one named last changes fastest.
Arguments:
- master_down: float32 [16, 6400, 4096], P('expert', None, 'shard'), may hold values from -0.109375 to 0.109375
- second_down: bfloat16 [16, 6400, 4096], P('expert', None, 'shard'), may hold values from -0.0390625 to 0.0390625
- router_weight: float32 [4096, 16], P('shard', 'expert'), may hold values from -0.09375 to 0.09375
- router_gain: float32 [4096], P('shard'), may hold values from 0.25 to 1.75
Outputs:
- final_down: bfloat16 [16, 6400, 4096], P('expert', 'shard')
- scale_down: float32 [16, 6400], P('expert', 'shard')
- serve_router: bfloat16 [4096, 16], replicated
The draws below stay inside these ranges and needn't reach their ends.
All inputs are finite; a program needn't handle non-finite values.
Results may differ from the reference program's by a relative error of at most 0.001.
Values may be sent and summed in bfloat16 or wider, within the bound.
A program may use at most 256 MiB of HBM per device.

```python
import jax
import jax.numpy as jnp
from jax import lax

EXPERTS = 16
D_MODEL = 4096
D_EXPERT = 6400


def spiked(values, stream_key, source, target, blocks, factor):
    def block_of(position):
        return (jnp.arange(values.shape[position]) // (values.shape[position] // blocks)).reshape((-1,) + (1,) * (values.ndim - 1 - position))

    one_side = jax.random.permutation(stream_key, blocks)[block_of(target)]
    other_side = (block_of(target) + blocks // 2) % blocks
    return jnp.where((block_of(source) == one_side) | (block_of(source) == other_side), factor * values, values)


def level_of(key, shape, split, low, top_value):
    loudness, own = 1.0, jax.random.fold_in(key, 6)
    for position, parts in split:
        draws = jnp.exp(jax.random.uniform(jax.random.fold_in(own, position), (parts,), jnp.float32, low / len(split), top_value / len(split)))
        loudness = loudness * jnp.repeat(draws, shape[position] // parts).reshape([-1 if axis == position else 1 for axis in range(len(shape))])
    return loudness


def bell_draw(key, shape, width, most, shards=(), kind=jnp.bfloat16):
    entries = width * jax.random.normal(key, shape, jnp.float32)
    if shards:
        entries = entries * level_of(key, shape, shards, -0.22, 0.18)
    return jnp.clip(entries, -most, most).astype(kind)


def bell_draw_with(rng, shape, scale, most, split, heavy, dtype=jnp.bfloat16):
    array = scale * jax.random.normal(rng, shape, jnp.float32)
    if split:
        array = array * level_of(rng, shape, split, -0.22, 0.18)
    return jnp.clip(spiked(array, jax.random.fold_in(rng, 3), *heavy), -most, most).astype(dtype)


def setup_inputs(seed: int = 0) -> dict:
    splits = jax.random.split(jax.random.key(seed), 5)
    return {
        "master_down": bell_draw_with(splits[0], (EXPERTS, D_EXPERT, D_MODEL), D_EXPERT ** -0.5, 0.109375, ((0, 4), (2, 8)), (2, 1, 8, 2.0), jnp.float32),
        "second_down": bell_draw(splits[1], (EXPERTS, D_EXPERT, D_MODEL), (D_EXPERT * 4) ** -0.5, 0.0390625, ((0, 4), (2, 8))),
        "router_weight": bell_draw(splits[2], (D_MODEL, EXPERTS), D_MODEL ** -0.5, 0.09375, ((0, 8), (1, 4)), jnp.float32),
        "router_gain": jnp.clip(1.0 + 0.15 * jax.random.normal(splits[3], (D_MODEL,), jnp.float32), 0.25, 1.75),
    }


def reference(master_down, second_down, router_weight, router_gain):
    merged_down = master_down + second_down.astype(jnp.float32)
    scale_down = jnp.sqrt(lax.optimization_barrier(jnp.sum(merged_down * merged_down, axis=2)))
    final_down = (merged_down / jnp.expand_dims(scale_down, 2)).astype(jnp.bfloat16)
    serve_router = (router_weight * router_gain[:, None]).astype(jnp.bfloat16)
    return (final_down, scale_down, serve_router)
```

```python
import functools

import jax
import jax.numpy as jnp
from jax import lax
from jax.experimental import pallas as pl
from jax.experimental.pallas import tpu as pltpu
from jax.sharding import PartitionSpec as P

MESH = pl.DeviceIdType.MESH
QUEUE = 3
READS = 3
SKEW = 2


def rows_per_chunk(rows):
    return max(r for r in range(16, 129, 16) if rows % r == 0)


def flipped(index, mask):
    out, bit = 0, 1
    while bit <= mask:
        own = lax.rem(index // bit, 2)
        if mask & bit:
            out = out + bit * (1 - 2 * own)
        bit *= 2
    return index + out


def kernel(
    shards, groups, master, second, weight, gain,
    final, scale, router,
    sum_master, sum_second, norm_master, norm_second, ready,
    part, landed, rpart, rall,
    sum_sems, norm_sems, send_sems, own_sems, final_sems,
    part_send, part_recv, rsend, rrecv, gsend, grecv,
):
    experts, _, rows, cols = master.shape
    take = rows_per_chunk(rows)
    blocks = rows // take
    chunks = experts * blocks
    stages = shards.bit_length() - 1
    me = lax.axis_index("shard")
    group = lax.axis_index("expert")
    lag = SKEW * stages

    def reads(k, bufs, sems):
        slot = lax.rem(k, READS)
        e, b = k // blocks, lax.rem(k, blocks)
        where = pl.ds(pl.multiple_of(b * take, 16), take)
        return [
            pltpu.make_async_copy(src.at[e, :, where, :], buf.at[slot], sems.at[i, slot])
            for i, (src, buf) in enumerate(zip((master, second), bufs))
        ]

    sum_bufs, norm_bufs = (sum_master, sum_second), (norm_master, norm_second)

    for k in range(min(READS, chunks)):
        for c in reads(k, sum_bufs, sum_sems):
            c.start()

    barrier = pltpu.get_barrier_semaphore()
    for o in range(1, shards):
        pl.semaphore_signal(barrier, inc=1, device_id={"shard": flipped(me, o)}, device_id_type=MESH)
    for o in range(1, groups):
        pl.semaphore_signal(barrier, inc=1, device_id={"expert": lax.rem(group + o, groups)}, device_id_type=MESH)

    product = (weight[...] * gain[...]).astype(jnp.bfloat16)
    rpart[...] = product
    mine = pl.ds(pl.multiple_of(me * cols, 128), cols)
    rall[group, :, mine] = product
    for k in range(min(READS, chunks)):
        for c in reads(k, norm_bufs, norm_sems):
            c.start()
    pl.semaphore_wait(barrier, shards + groups - 2)

    def exchange(stage, k):
        return pltpu.make_async_remote_copy(
            src_ref=part.at[stage, k],
            dst_ref=landed.at[stage, k],
            send_sem=part_send.at[stage],
            recv_sem=part_recv.at[stage, k],
            device_id={"shard": flipped(me, 1 << stage)},
            device_id_type=MESH,
        )

    eye = lax.broadcasted_iota(jnp.int32, (take, 128), 0) == lax.broadcasted_iota(jnp.int32, (take, 128), 1)

    def send(k, o):
        slot = lax.rem(k, QUEUE)
        e, b = k // blocks, lax.rem(k, blocks)
        where = pl.ds(pl.multiple_of(b * take, 16), take)
        to = flipped(me, o)
        return pltpu.make_async_remote_copy(
            src_ref=ready.at[slot, to],
            dst_ref=final.at[e, where, mine],
            send_sem=send_sems.at[slot],
            recv_sem=final_sems.at[me],
            device_id={"shard": to},
            device_id_type=MESH,
        )

    def keep(k):
        slot = lax.rem(k, QUEUE)
        e, b = k // blocks, lax.rem(k, blocks)
        where = pl.ds(pl.multiple_of(b * take, 16), take)
        return pltpu.make_async_copy(ready.at[slot, me], final.at[e, where, mine], own_sems.at[slot])

    def drain(k):
        slot = lax.rem(k, QUEUE)
        several = ready.at[slot, pl.ds(0, shards - 1)]
        pltpu.make_async_copy(several, several, send_sems.at[slot]).wait()
        keep(k).wait()

    def tick(t, carry):
        @pl.when(t < chunks)
        def _():
            slot = lax.rem(t, READS)
            for c in reads(t, sum_bufs, sum_sems):
                c.wait()

            def one(d, carry):
                x = sum_master[slot, d] + sum_second[slot, d].astype(jnp.float32)
                column = jnp.sum(x * x, axis=1, keepdims=True)
                part[0, t, pl.ds(d, 1), :] = jnp.sum(jnp.where(eye, column, 0.0), axis=0, keepdims=True)
                return carry

            lax.fori_loop(0, shards, one, 0, unroll=2)

            @pl.when(t + READS < chunks)
            def _():
                for c in reads(t + READS, sum_bufs, sum_sems):
                    c.start()

        for stage in range(1, stages):
            k = t - SKEW * stage

            @pl.when((k >= 0) & (k < chunks))
            def _():
                exchange(stage - 1, k).wait_recv()
                part[stage, k] = part[stage - 1, k] + landed[stage - 1, k]

        for stage in range(stages):
            k = t - SKEW * stage

            @pl.when((k >= 0) & (k < chunks))
            def _():
                exchange(stage, k).start()

        k = t - lag

        @pl.when((k >= 0) & (k < chunks))
        def _():
            slot = lax.rem(k, READS)
            out = lax.rem(k, QUEUE)
            exchange(stages - 1, k).wait_recv()
            part[stages, k] = jnp.sqrt(part[stages - 1, k] + landed[stages - 1, k])
            scale[pl.ds(k, 1), :] = part[stages, k, pl.ds(me, 1), :]
            for c in reads(k, norm_bufs, norm_sems):
                c.wait()

            @pl.when(k >= QUEUE)
            def _():
                drain(k - QUEUE)

            def one(d, carry):
                row = 1.0 / part[stages, k, pl.ds(d, 1), :]
                column = jnp.sum(jnp.where(eye, row, 0.0), axis=1, keepdims=True)
                x = norm_master[slot, d] + norm_second[slot, d].astype(jnp.float32)
                ready[out, d] = (x * column).astype(jnp.bfloat16)
                return carry

            lax.fori_loop(0, shards, one, 0, unroll=2)

            @pl.when(k + READS < chunks)
            def _():
                for c in reads(k + READS, norm_bufs, norm_sems):
                    c.start()

            for o in range(shards - 1, 0, -1):
                send(k, o).start()
            keep(k).start()

        return carry

    def rows_copy(o):
        return pltpu.make_async_remote_copy(
            src_ref=rpart,
            dst_ref=rall.at[group, :, mine],
            send_sem=rsend,
            recv_sem=rrecv.at[me],
            device_id={"shard": flipped(me, o)},
            device_id_type=MESH,
        )

    for o in range(1, shards):
        rows_copy(o).start()

    lax.fori_loop(0, chunks + lag, tick, 0)

    def group_copy(o):
        return pltpu.make_async_remote_copy(
            src_ref=rall.at[group],
            dst_ref=rall.at[group],
            send_sem=gsend.at[o],
            recv_sem=grecv.at[group],
            device_id={"expert": lax.rem(group + o, groups)},
            device_id_type=MESH,
        )

    for o in range(1, shards):
        rows_copy(o).wait_send()
        other = flipped(me, o)
        there = rall.at[group, :, pl.ds(pl.multiple_of(other * cols, 128), cols)]
        pltpu.make_async_copy(there, there, rrecv.at[other]).wait()
    for o in range(1, groups):
        group_copy(o).start()
    for o in range(1, groups):
        other = lax.rem(group + o, groups)
        pltpu.make_async_copy(rall.at[other], rall.at[other], grecv.at[other]).wait()
        group_copy(o).wait_send()
    router[...] = rall[...]

    for stage in range(stages):
        pltpu.make_async_copy(part.at[stage], part.at[stage], part_send.at[stage]).wait()
    for k in range(max(0, chunks - QUEUE), chunks):
        drain(k)
    for o in range(1, shards):
        other = flipped(me, o)
        there = final.at[:, :, pl.ds(pl.multiple_of(other * cols, 128), cols)]
        pltpu.make_async_copy(there, there, final_sems.at[other]).wait()


def local(shards, groups, master_down, second_down, router_weight, router_gain):
    experts, d_expert, cols = master_down.shape
    rows = d_expert // shards
    take = rows_per_chunk(rows)
    chunks = experts * (rows // take)
    stages = shards.bit_length() - 1
    gcols = router_weight.shape[1]
    f32, bf16 = jnp.float32, jnp.bfloat16
    final, scale, router = pl.pallas_call(
        functools.partial(kernel, shards, groups),
        out_shape=(
            jax.ShapeDtypeStruct((experts, rows, cols * shards), bf16),
            jax.ShapeDtypeStruct((chunks, 128), f32),
            jax.ShapeDtypeStruct((groups, gcols, cols * shards), bf16),
        ),
        in_specs=[pl.BlockSpec(memory_space=pl.ANY)] * 2 + [pl.BlockSpec(memory_space=pltpu.VMEM)] * 2,
        out_specs=(
            pl.BlockSpec(memory_space=pl.ANY),
            pl.BlockSpec(memory_space=pltpu.VMEM),
            pl.BlockSpec(memory_space=pltpu.VMEM),
        ),
        scratch_shapes=[
            pltpu.VMEM((READS, shards, take, cols), f32),
            pltpu.VMEM((READS, shards, take, cols), bf16),
            pltpu.VMEM((READS, shards, take, cols), f32),
            pltpu.VMEM((READS, shards, take, cols), bf16),
            pltpu.VMEM((QUEUE, shards, take, cols), bf16),
            pltpu.VMEM((stages + 1, chunks, shards, 128), f32),
            pltpu.VMEM((stages, chunks, shards, 128), f32),
            pltpu.VMEM((gcols, cols), bf16),
            pltpu.VMEM((groups, gcols, cols * shards), bf16),
            pltpu.SemaphoreType.DMA((2, READS)),
            pltpu.SemaphoreType.DMA((2, READS)),
            pltpu.SemaphoreType.DMA((QUEUE,)),
            pltpu.SemaphoreType.DMA((QUEUE,)),
            pltpu.SemaphoreType.DMA((shards,)),
            pltpu.SemaphoreType.DMA((stages,)),
            pltpu.SemaphoreType.DMA((stages, chunks)),
            pltpu.SemaphoreType.DMA,
            pltpu.SemaphoreType.DMA((shards,)),
            pltpu.SemaphoreType.DMA((groups,)),
            pltpu.SemaphoreType.DMA((groups,)),
        ],
        compiler_params=pltpu.CompilerParams(collective_id=0, has_side_effects=True, vmem_limit_bytes=32 * 2**20),
    )(
        master_down.reshape(experts, shards, rows, cols),
        second_down.reshape(experts, shards, rows, cols),
        router_weight.T,
        router_gain[None, :],
    )
    scale = scale[:, :take].reshape(experts, rows)
    return (final, scale, router.reshape(groups * gcols, cols * shards).T)


def solution(mesh):
    shards, groups = mesh.shape["shard"], mesh.shape["expert"]
    return jax.shard_map(
        functools.partial(local, shards, groups),
        mesh=mesh,
        in_specs=(
            P("expert", None, "shard"),
            P("expert", None, "shard"),
            P("shard", "expert"),
            P("shard"),
        ),
        out_specs=(P("expert", "shard", None), P("expert", "shard"), P()),
        check_vma=False,
    )
```

```python
import functools

import jax
import jax.numpy as jnp
from jax import lax
from jax.experimental import pallas as pl
from jax.experimental.pallas import tpu as pltpu
from jax.sharding import PartitionSpec as P

MESH = pl.DeviceIdType.MESH
QUEUE = 3
READS = 3
SKEW = 1


def rows_per_chunk(rows):
    return max(r for r in range(16, 129, 16) if rows % r == 0)


def flipped(index, mask):
    out, bit = 0, 1
    while bit <= mask:
        own = lax.rem(index // bit, 2)
        if mask & bit:
            out = out + bit * (1 - 2 * own)
        bit *= 2
    return index + out


def kernel(
    shards, groups, master, second, weight, gain,
    final, scale, router,
    sum_master, sum_second, norm_master, norm_second, ready,
    part, landed, rpart, rall,
    sum_sems, norm_sems, send_sems, own_sems, final_sems,
    part_send, part_recv, rsend, rrecv, gsend, grecv,
    weight_here, gain_here, small_sems,
):
    experts, _, rows, cols = master.shape
    take = rows_per_chunk(rows)
    blocks = rows // take
    chunks = experts * blocks
    stages = shards.bit_length() - 1
    me = lax.axis_index("shard")
    group = lax.axis_index("expert")
    lag = SKEW * stages

    def reads(k, bufs, sems):
        slot = lax.rem(k, READS)
        e, b = k // blocks, lax.rem(k, blocks)
        where = pl.ds(pl.multiple_of(b * take, 16), take)
        return [
            pltpu.make_async_copy(src.at[e, :, where, :], buf.at[slot], sems.at[i, slot])
            for i, (src, buf) in enumerate(zip((master, second), bufs))
        ]

    sum_bufs, norm_bufs = (sum_master, sum_second), (norm_master, norm_second)

    for k in range(min(READS, chunks)):
        for c in reads(k, sum_bufs, sum_sems):
            c.start()

    small = [
        pltpu.make_async_copy(weight, weight_here, small_sems.at[0]),
        pltpu.make_async_copy(gain, gain_here, small_sems.at[1]),
    ]
    for c in small:
        c.start()
    barrier = pltpu.get_barrier_semaphore()
    for o in range(1, shards):
        pl.semaphore_signal(barrier, inc=1, device_id={"shard": flipped(me, o)}, device_id_type=MESH)
    for o in range(1, groups):
        pl.semaphore_signal(barrier, inc=1, device_id={"expert": lax.rem(group + o, groups)}, device_id_type=MESH)

    for c in small:
        c.wait()
    product = (weight_here[...] * gain_here[...]).astype(jnp.bfloat16)
    rpart[...] = product
    mine = pl.ds(pl.multiple_of(me * cols, 128), cols)
    rall[group, :, mine] = product
    for k in range(min(READS, chunks)):
        for c in reads(k, norm_bufs, norm_sems):
            c.start()
    pl.semaphore_wait(barrier, shards + groups - 2)

    def exchange(stage, k):
        return pltpu.make_async_remote_copy(
            src_ref=part.at[stage, k],
            dst_ref=landed.at[stage, k],
            send_sem=part_send.at[stage],
            recv_sem=part_recv.at[stage, k],
            device_id={"shard": flipped(me, 1 << stage)},
            device_id_type=MESH,
        )

    eye = lax.broadcasted_iota(jnp.int32, (take, 128), 0) == lax.broadcasted_iota(jnp.int32, (take, 128), 1)

    def send(k, o):
        slot = lax.rem(k, QUEUE)
        e, b = k // blocks, lax.rem(k, blocks)
        where = pl.ds(pl.multiple_of(b * take, 16), take)
        to = flipped(me, o)
        return pltpu.make_async_remote_copy(
            src_ref=ready.at[slot, to],
            dst_ref=final.at[e, where, mine],
            send_sem=send_sems.at[slot],
            recv_sem=final_sems.at[me],
            device_id={"shard": to},
            device_id_type=MESH,
        )

    def keep(k):
        slot = lax.rem(k, QUEUE)
        e, b = k // blocks, lax.rem(k, blocks)
        where = pl.ds(pl.multiple_of(b * take, 16), take)
        return pltpu.make_async_copy(ready.at[slot, me], final.at[e, where, mine], own_sems.at[slot])

    def drain(k):
        slot = lax.rem(k, QUEUE)
        several = ready.at[slot, pl.ds(0, shards - 1)]
        pltpu.make_async_copy(several, several, send_sems.at[slot]).wait()
        keep(k).wait()

    def tick(t, carry):
        @pl.when(t < chunks)
        def _():
            slot = lax.rem(t, READS)
            for c in reads(t, sum_bufs, sum_sems):
                c.wait()

            def one(d, carry):
                x = sum_master[slot, d] + sum_second[slot, d].astype(jnp.float32)
                column = jnp.sum(x * x, axis=1, keepdims=True)
                part[0, t, pl.ds(d, 1), :] = jnp.sum(jnp.where(eye, column, 0.0), axis=0, keepdims=True)
                return carry

            lax.fori_loop(0, shards, one, 0, unroll=2)

            @pl.when(t + READS < chunks)
            def _():
                for c in reads(t + READS, sum_bufs, sum_sems):
                    c.start()

        for stage in range(1, stages):
            k = t - SKEW * stage

            @pl.when((k >= 0) & (k < chunks))
            def _():
                exchange(stage - 1, k).wait_recv()
                part[stage, k] = part[stage - 1, k] + landed[stage - 1, k]

        for stage in range(stages):
            k = t - SKEW * stage

            @pl.when((k >= 0) & (k < chunks))
            def _():
                exchange(stage, k).start()

        k = t - lag

        @pl.when((k >= 0) & (k < chunks))
        def _():
            slot = lax.rem(k, READS)
            out = lax.rem(k, QUEUE)
            exchange(stages - 1, k).wait_recv()
            part[stages, k] = jnp.sqrt(part[stages - 1, k] + landed[stages - 1, k])
            scale[pl.ds(k, 1), :] = part[stages, k, pl.ds(me, 1), :]
            for c in reads(k, norm_bufs, norm_sems):
                c.wait()

            @pl.when(k >= QUEUE)
            def _():
                drain(k - QUEUE)

            def one(d, carry):
                row = 1.0 / part[stages, k, pl.ds(d, 1), :]
                column = jnp.sum(jnp.where(eye, row, 0.0), axis=1, keepdims=True)
                x = norm_master[slot, d] + norm_second[slot, d].astype(jnp.float32)
                ready[out, d] = (x * column).astype(jnp.bfloat16)
                return carry

            lax.fori_loop(0, shards, one, 0, unroll=2)

            @pl.when(k + READS < chunks)
            def _():
                for c in reads(k + READS, norm_bufs, norm_sems):
                    c.start()

            for o in range(shards - 1, 0, -1):
                send(k, o).start()
            keep(k).start()

        return carry

    def rows_copy(o):
        return pltpu.make_async_remote_copy(
            src_ref=rpart,
            dst_ref=rall.at[group, :, mine],
            send_sem=rsend,
            recv_sem=rrecv.at[me],
            device_id={"shard": flipped(me, o)},
            device_id_type=MESH,
        )

    for o in range(1, shards):
        rows_copy(o).start()

    lax.fori_loop(0, chunks + lag, tick, 0)

    def group_copy(o):
        return pltpu.make_async_remote_copy(
            src_ref=rall.at[group],
            dst_ref=rall.at[group],
            send_sem=gsend.at[o],
            recv_sem=grecv.at[group],
            device_id={"expert": lax.rem(group + o, groups)},
            device_id_type=MESH,
        )

    for o in range(1, shards):
        rows_copy(o).wait_send()
        other = flipped(me, o)
        there = rall.at[group, :, pl.ds(pl.multiple_of(other * cols, 128), cols)]
        pltpu.make_async_copy(there, there, rrecv.at[other]).wait()
    for o in range(1, groups):
        group_copy(o).start()
    for o in range(1, groups):
        other = lax.rem(group + o, groups)
        pltpu.make_async_copy(rall.at[other], rall.at[other], grecv.at[other]).wait()
        group_copy(o).wait_send()
    router[...] = rall[...]

    for stage in range(stages):
        pltpu.make_async_copy(part.at[stage], part.at[stage], part_send.at[stage]).wait()
    for k in range(max(0, chunks - QUEUE), chunks):
        drain(k)
    for o in range(1, shards):
        other = flipped(me, o)
        there = final.at[:, :, pl.ds(pl.multiple_of(other * cols, 128), cols)]
        pltpu.make_async_copy(there, there, final_sems.at[other]).wait()


def local(shards, groups, master_down, second_down, router_weight, router_gain):
    experts, d_expert, cols = master_down.shape
    rows = d_expert // shards
    take = rows_per_chunk(rows)
    chunks = experts * (rows // take)
    stages = shards.bit_length() - 1
    gcols = router_weight.shape[1]
    f32, bf16 = jnp.float32, jnp.bfloat16
    final, scale, router = pl.pallas_call(
        functools.partial(kernel, shards, groups),
        out_shape=(
            jax.ShapeDtypeStruct((experts, rows, cols * shards), bf16),
            jax.ShapeDtypeStruct((chunks, 128), f32),
            jax.ShapeDtypeStruct((groups, gcols, cols * shards), bf16),
        ),
        in_specs=[pl.BlockSpec(memory_space=pl.ANY)] * 2 + [pl.BlockSpec(memory_space=pltpu.HBM)] * 2,
        out_specs=(
            pl.BlockSpec(memory_space=pl.ANY),
            pl.BlockSpec(memory_space=pltpu.VMEM),
            pl.BlockSpec(memory_space=pltpu.VMEM),
        ),
        scratch_shapes=[
            pltpu.VMEM((READS, shards, take, cols), f32),
            pltpu.VMEM((READS, shards, take, cols), bf16),
            pltpu.VMEM((READS, shards, take, cols), f32),
            pltpu.VMEM((READS, shards, take, cols), bf16),
            pltpu.VMEM((QUEUE, shards, take, cols), bf16),
            pltpu.VMEM((stages + 1, chunks, shards, 128), f32),
            pltpu.VMEM((stages, chunks, shards, 128), f32),
            pltpu.VMEM((gcols, cols), bf16),
            pltpu.VMEM((groups, gcols, cols * shards), bf16),
            pltpu.SemaphoreType.DMA((2, READS)),
            pltpu.SemaphoreType.DMA((2, READS)),
            pltpu.SemaphoreType.DMA((QUEUE,)),
            pltpu.SemaphoreType.DMA((QUEUE,)),
            pltpu.SemaphoreType.DMA((shards,)),
            pltpu.SemaphoreType.DMA((stages,)),
            pltpu.SemaphoreType.DMA((stages, chunks)),
            pltpu.SemaphoreType.DMA,
            pltpu.SemaphoreType.DMA((shards,)),
            pltpu.SemaphoreType.DMA((groups,)),
            pltpu.SemaphoreType.DMA((groups,)),
            pltpu.VMEM((gcols, cols), f32),
            pltpu.VMEM((1, cols), f32),
            pltpu.SemaphoreType.DMA((2,)),
        ],
        compiler_params=pltpu.CompilerParams(collective_id=0, has_side_effects=True, vmem_limit_bytes=32 * 2**20),
    )(
        master_down.reshape(experts, shards, rows, cols),
        second_down.reshape(experts, shards, rows, cols),
        router_weight.T,
        router_gain[None, :],
    )
    scale = scale[:, :take].reshape(experts, rows)
    return (final, scale, router.reshape(groups * gcols, cols * shards).T)


def solution(mesh):
    shards, groups = mesh.shape["shard"], mesh.shape["expert"]
    return jax.shard_map(
        functools.partial(local, shards, groups),
        mesh=mesh,
        in_specs=(
            P("expert", None, "shard"),
            P("expert", None, "shard"),
            P("shard", "expert"),
            P("shard"),
        ),
        out_specs=(P("expert", "shard", None), P("expert", "shard"), P()),
        check_vma=False,
    )
```
